32 devices in a mesh: samp: 8 (over y, x, core), cpg: 4 (over z).
Axes of the slice: x: 2, y: 2, z: 4, core: 2. Of those that a mesh axis runs over, the one named last changes fastest.
Arguments:
- responses: bfloat16 [256, 16384], P('samp', 'cpg'), may hold values from -5 to 5
- weights: bfloat16 [256, 16384], P('samp', 'cpg'), may hold values from 1 to 8
- phenotype: float32 [16384], P('cpg'), may hold values from -6 to 6
- eigvecs: bfloat16 [16384, 16384], P('cpg', 'samp'), may hold values from -0.046875 to 0.046875
- eigvals: float32 [16384], P('samp'), may hold values from 0.0001 to 1
- positions: int32 [256], replicated, may hold values from 1 to 76800, as said below
- reaches: int32 [256], P('cpg'), may hold values from 1 to 8
Outputs:
- smoothed: float32 [256], P('cpg')
- log_scale: float32 [256], P('cpg')
The draws below stay inside these ranges and needn't reach their ends.
Inputs may be any that keep to these rules, and one draw needn't show every extreme that they name: CpG m (from 0) lies at 300 m plus an offset of 1 to 300, so positions strictly increase and consecutive CpGs lie 1 to 599 base pairs apart.
All inputs are finite; a program needn't handle non-finite values.
Results may differ from the reference program's by a relative error of at most 0.0041.
Values may be sent and summed in bfloat16 or wider, within the bound.
A program may use at most 64 MiB of HBM per device.

```python
import math
import jax
import jax.numpy as jnp
from jax import lax

N = 16384
ITERS = 4
HALO = 8
M = 256


def draw_positions(key, part):
    offsets = jax.random.randint(key, (M,), 1, 301)
    index = jnp.arange(M, dtype=jnp.int32)
    offsets = jnp.where(index == 0, 1, offsets)
    offsets = jnp.where(index == M - 1, 300, offsets)
    return (300 * index + offsets).astype(jnp.int32)


def draw_working(key):
    root_key = jax.random.fold_in(key, 4049)
    weight_key = jax.random.fold_in(root_key, 1)
    noise_key = jax.random.fold_in(root_key, 2)
    excess_key = jax.random.fold_in(root_key, 3)
    weight_draw = jnp.exp(jax.random.uniform(weight_key, (M, N), jnp.float32, 0.0, jnp.log(8.0)))
    noise_draw = jnp.clip(jax.random.normal(noise_key, (M, N), jnp.float32), -4.0, 4.0)
    weight_draw = jnp.clip(weight_draw, 1.0, 8.0).astype(jnp.bfloat16)
    excess = 0.04 * jnp.exp(jax.random.uniform(excess_key, (M, 1), jnp.float32, 0.0, jnp.log(5.0)))
    row_scale = jnp.sqrt((1.0 + excess) / weight_draw.astype(jnp.float32))
    response_draw = jnp.clip(row_scale * noise_draw, -5.0, 5.0).astype(jnp.bfloat16)
    return (weight_draw, response_draw)


def draw_weights(key, part):
    return draw_working(key)[0]


def draw_responses(key, part):
    return draw_working(key)[1]


def plant(array, stream_key, smallest, top_value):
    spot = [jax.random.randint(jax.random.fold_in(stream_key, axis), (), 0, length) for axis, length in enumerate(array.shape)]
    widest = array.shape.index(max(array.shape))
    neighbour = spot[:widest] + [(spot[widest] + 1) % array.shape[widest]] + spot[widest + 1:]
    return array.at[tuple(spot)].set(smallest).at[tuple(neighbour)].set(top_value)


def steps_of(key, extent, split, low, high):
    factor_of = 1.0
    for axis_at, blocks in split:
        draws = jax.random.uniform(jax.random.fold_in(jax.random.fold_in(key, 6), axis_at), (blocks,), jnp.float32, low / len(split), high / len(split))
        factor_of = factor_of * jnp.repeat(jnp.exp(draws), extent[axis_at] // blocks).reshape((-1,) + (1,) * (len(extent) - 1 - axis_at))
    return factor_of


def noise(stream_key, shape, scale, most, shards=(), kind=jnp.bfloat16):
    array = scale * jax.random.normal(stream_key, shape, jnp.float32)
    if shards:
        array = array * steps_of(stream_key, shape, shards, -0.22, 0.18)
    return jnp.clip(array, -most, most).astype(kind)


def setup_inputs(seed: int = 0) -> dict:
    key_of = jax.random.split(jax.random.key(seed), 8)
    return {
        "responses": draw_responses(jax.random.fold_in(key_of[7], 71), 0),
        "weights": draw_weights(jax.random.fold_in(key_of[7], 71), 0),
        "phenotype": noise(key_of[2], (N,), 1.0, 6.0, ((0, 4),), jnp.float32),
        "eigvecs": noise(key_of[3], (N, N), N ** -0.5, 0.046875, ((0, 4), (1, 8))),
        "eigvals": jnp.clip(jnp.exp(math.log(1.0) - 9.2103404 * jax.random.uniform(key_of[4], (N,), jnp.float32) ** steps_of(key_of[4], (N,), ((0, 8),), -0.2, 0.2)), 0.0001, 1.0),
        "positions": draw_positions(jax.random.fold_in(key_of[7], 71), 0),
        "reaches": plant(jax.random.randint(key_of[6], (M,), 1, HALO + 1), jax.random.fold_in(key_of[6], 1), 1, HALO).astype(jnp.int32),
    }


EPSILON = 1e-06
band_width = 1000.0

def smooth_block(widened, places, present, reaches):
    block_len = reaches.shape[0]
    centre = places[HALO:HALO + block_len]
    total_sum = jnp.zeros((block_len,), jnp.float32)
    norm_sum = jnp.zeros((block_len,), jnp.float32)
    for offset in range(2 * HALO + 1):
        near_scores = widened[offset:offset + block_len]
        near_places = places[offset:offset + block_len]
        within = (abs(offset - HALO) <= reaches).astype(jnp.float32)
        kernel = present[offset:offset + block_len] * within * jnp.exp(-jnp.abs(near_places - centre) / band_width)
        total_sum = total_sum + kernel * near_scores
        norm_sum = norm_sum + kernel
    return total_sum / norm_sum

def reference(responses, weights, phenotype, eigvecs, eigvals, positions, reaches):
    root_weight = jnp.sqrt(weights.astype(jnp.float32))
    weighted = (root_weight * responses.astype(jnp.float32)).astype(jnp.bfloat16)
    design = (root_weight * phenotype[None, :]).astype(jnp.bfloat16)
    rot_resp = jnp.dot(weighted, eigvecs, preferred_element_type=jnp.float32)
    rot_design = jnp.dot(design, eigvecs, preferred_element_type=jnp.float32)
    eigen_part = eigvals[None, :]
    log_scale = jnp.zeros((M,), jnp.float32)
    for repeat in range(ITERS):
        inverse = 1.0 / (jnp.exp(log_scale)[:, None] * eigen_part + 1.0)
        crossed = lax.optimization_barrier(jnp.sum(rot_design * rot_resp * inverse, axis=1))
        energy = lax.optimization_barrier(jnp.sum(rot_design * rot_design * inverse, axis=1)) + EPSILON
        effect = crossed / energy
        residual = rot_resp - effect[:, None] * rot_design
        spread = lax.optimization_barrier(jnp.sum(eigen_part * residual * residual * inverse * inverse, axis=1))
        traced = lax.optimization_barrier(jnp.sum(eigen_part * inverse, axis=1))
        fisher = 0.5 * lax.optimization_barrier(jnp.sum(eigen_part * eigen_part * inverse * inverse, axis=1))
        gradient = 0.5 * (spread - traced)
        log_scale = log_scale + jnp.tanh(gradient / (jnp.exp(log_scale) * fisher))
    inverse = 1.0 / (jnp.exp(log_scale)[:, None] * eigen_part + 1.0)
    crossed = lax.optimization_barrier(jnp.sum(rot_design * rot_resp * inverse, axis=1))
    energy = lax.optimization_barrier(jnp.sum(rot_design * rot_design * inverse, axis=1)) + EPSILON
    zscore = crossed / jnp.sqrt(energy)
    widened = jnp.pad(zscore, HALO)
    places = jnp.pad(positions.astype(jnp.float32), HALO)
    present = jnp.pad(jnp.ones((M,), jnp.float32), HALO)
    smoothed = smooth_block(widened, places, present, reaches)
    return (smoothed, log_scale)
```

```python
import functools

import jax
import jax.numpy as jnp
from jax import lax
from jax.experimental import pallas as pl
from jax.experimental.pallas import tpu as pltpu
from jax.sharding import PartitionSpec as P

ITERS = 4
HALO = 8
EPSILON = 1e-06
band_width = 1000.0
MESH = pl.DeviceIdType.MESH
LANES = 128


def fit_kernel(n, cpgs, a_ref, b_ref, lam_ref, band_ref, out_ref, p_ref, q_ref, r_ref, l_ref, send, recv, edge, zsend, ssem, rsem, esem, fsem):
    me = lax.axis_index("samp")
    mz = lax.axis_index("cpg")
    block = a_ref.shape[0]
    fold = LANES // block
    rows = a_ref.shape[1] // fold
    edge[...] = jnp.zeros_like(edge)

    barrier = pltpu.get_barrier_semaphore()
    for j in range(1, n):
        pl.semaphore_signal(barrier, inc=1, device_id={"samp": lax.rem(me + j, n)}, device_id_type=MESH)

    for other in (lax.rem(mz + 1, cpgs), lax.rem(mz + cpgs - 1, cpgs)):
        pl.semaphore_signal(barrier, inc=1, device_id={"cpg": other}, device_id_type=MESH)

    def folded(ref):
        parts = [ref[:, pl.ds(g * rows, rows)].astype(jnp.float32) for g in range(fold)]
        return jnp.concatenate(parts, axis=0).T

    a = folded(a_ref)
    b = folded(b_ref)
    p_ref[...] = a * b
    q_ref[...] = b * b
    r_ref[...] = a * a
    lam_parts = [jnp.broadcast_to(lam_ref[:, pl.ds(g * rows, rows)], (block, rows)) for g in range(fold)]
    l_ref[...] = jnp.concatenate(lam_parts, axis=0).T

    pl.semaphore_wait(barrier, n + 1)

    step = 64

    def sums(log_scale, full):
        scale = jnp.exp(log_scale)

        def body(i, acc):
            at = pl.ds(pl.multiple_of(i * step, step), step)
            lam = l_ref[at, :]
            inv = 1.0 / (scale * lam + 1.0)
            p = p_ref[at, :]
            q = q_ref[at, :]
            terms = [p * inv, q * inv]
            if full:
                lev = lam * inv
                s = lev * inv
                terms += [lev, lev * lev, s * r_ref[at, :], s * p, s * q]
            terms = [t.reshape(step // 8, 8, LANES).sum(axis=0) for t in terms]
            return tuple(x + y for x, y in zip(acc, terms))

        count = 7 if full else 2
        acc = lax.fori_loop(0, rows // step, body, tuple(jnp.zeros((8, LANES), jnp.float32) for _ in range(count)))
        flat = []
        for x in acc:
            row = jnp.sum(x, axis=0, keepdims=True)
            total = row
            for g in range(1, fold):
                total = total + pltpu.roll(row, g * block, 1)
            flat.append(total)
        flat += [jnp.zeros((1, LANES), jnp.float32)] * (8 - count)
        return jnp.concatenate(flat, axis=0)

    def total(it, value):
        send[it] = value
        copies = []
        for j in range(1, n):
            copies.append(pltpu.make_async_remote_copy(
                src_ref=send.at[it], dst_ref=recv.at[it, j],
                send_sem=ssem.at[it, j], recv_sem=rsem.at[it, j],
                device_id={"samp": lax.rem(me + j, n)}, device_id_type=MESH))
        for c in copies:
            c.start()
        recv[it, 0] = value
        for c in copies:
            c.wait_recv()
        out = jnp.zeros((8, LANES), jnp.float32)
        for d in range(n):
            out = out + recv[it, lax.rem(me - d + n, n)]
        for c in copies:
            c.wait_send()
        return out

    log_scale = jnp.zeros((1, LANES), jnp.float32)
    for it in range(ITERS):
        t = total(it, sums(log_scale, True))
        crossed, energy, traced, fisher = t[0:1], t[1:2] + EPSILON, t[2:3], t[3:4]
        effect = crossed / energy
        spread = t[4:5] - 2.0 * effect * t[5:6] + effect * effect * t[6:7]
        gradient = 0.5 * (spread - traced)
        log_scale = log_scale + jnp.tanh(gradient / (jnp.exp(log_scale) * (0.5 * fisher)))
    t = total(ITERS, sums(log_scale, False))
    z = t[0:1] / jnp.sqrt(t[1:2] + EPSILON)
    z = jnp.broadcast_to(z, (8, LANES))
    zsend[...] = z
    down = pltpu.make_async_remote_copy(
        src_ref=zsend, dst_ref=edge.at[1], send_sem=esem.at[0], recv_sem=fsem.at[1],
        device_id={"cpg": lax.max(mz - 1, 0)}, device_id_type=MESH)
    up = pltpu.make_async_remote_copy(
        src_ref=zsend, dst_ref=edge.at[0], send_sem=esem.at[1], recv_sem=fsem.at[0],
        device_id={"cpg": lax.min(mz + 1, cpgs - 1)}, device_id_type=MESH)

    @pl.when(mz > 0)
    def _():
        down.start()

    @pl.when(mz < cpgs - 1)
    def _():
        up.start()

    @pl.when(mz > 0)
    def _():
        down.wait_send()
        up.wait_recv()

    @pl.when(mz < cpgs - 1)
    def _():
        up.wait_send()
        down.wait_recv()

    lane = lax.broadcasted_iota(jnp.int32, (8, LANES), 1)
    wide = jnp.where(lane < block, z, jnp.where(lane < block + HALO, edge[1], edge[0]))
    acc = jnp.zeros((8, LANES), jnp.float32)
    norm = jnp.zeros((8, LANES), jnp.float32)
    for o in range(2 * HALO + 1):
        shift = (HALO - o) % LANES
        near = pltpu.roll(wide, shift, 1) if shift else wide
        c = band_ref[o : o + 1, :]
        acc = acc + c * near
        norm = norm + c
    row = lax.broadcasted_iota(jnp.int32, (8, LANES), 0)
    out_ref[...] = jnp.where(row == 0, acc / norm, jnp.broadcast_to(log_scale, (8, LANES)))


def fit(a, b, lam, band, n, cpgs):
    block, comps = a.shape
    fold = LANES // block
    rows = comps // fold
    big = pltpu.VMEM((rows, LANES), jnp.float32)
    return pl.pallas_call(
        functools.partial(fit_kernel, n, cpgs),
        out_shape=jax.ShapeDtypeStruct((8, LANES), jnp.float32),
        in_specs=[pl.BlockSpec(memory_space=pltpu.VMEM)] * 4,
        out_specs=pl.BlockSpec(memory_space=pltpu.VMEM),
        scratch_shapes=[
            big, big, big, big,
            pltpu.VMEM((ITERS + 1, 8, LANES), jnp.float32),
            pltpu.VMEM((ITERS + 1, n, 8, LANES), jnp.float32),
            pltpu.VMEM((2, 8, LANES), jnp.float32),
            pltpu.VMEM((8, LANES), jnp.float32),
            pltpu.SemaphoreType.DMA((ITERS + 1, n)),
            pltpu.SemaphoreType.DMA((ITERS + 1, n)),
            pltpu.SemaphoreType.DMA((2,)),
            pltpu.SemaphoreType.DMA((2,)),
        ],
        compiler_params=pltpu.CompilerParams(collective_id=1, has_side_effects=True),
        cost_estimate=pl.CostEstimate(flops=20_000_000, bytes_accessed=2_000_000, transcendentals=0),
        name="fit",
    )(a, b, lam, band)


CHUNK = 256


def rotate_kernel(n, cpgs, w_ref, d_ref, v_hbm, a_ref, b_ref, g, v, part, sent, below, above, vsem, gs, gr, ss, bs, us):
    me = lax.axis_index("samp")
    mz = lax.axis_index("cpg")
    each = w_ref.shape[0]
    total = each * n
    block = total // cpgs
    chunks = v.shape[0]
    bits = [1 << i for i in range(1, n.bit_length() - 1)]
    orders = (bits, bits[::-1])
    inputs = (w_ref, d_ref)

    def load(c):
        return pltpu.make_async_copy(v_hbm.at[:, pl.ds(pl.multiple_of(c * CHUNK, CHUNK), CHUNK)], v.at[c], vsem.at[c])

    for c in range(chunks):
        load(c).start()

    def flipped(mask):
        out = me
        bit = 1
        while bit <= mask:
            if mask & bit:
                out = out + bit - 2 * bit * lax.rem(lax.div(me, bit), 2)
            bit *= 2
        return out

    barrier = pltpu.get_barrier_semaphore()
    for bit in [1] + bits:
        pl.semaphore_signal(barrier, inc=1, device_id={"samp": flipped(bit)}, device_id_type=MESH)
    for other in (lax.rem(mz + 1, cpgs), lax.rem(mz + cpgs - 1, cpgs)):
        pl.semaphore_signal(barrier, inc=1, device_id={"cpg": other}, device_id_type=MESH)
    for k in range(2):
        g[pl.ds(pl.multiple_of(k * total + me * each, each), each), :] = inputs[k][...]
    pl.semaphore_wait(barrier, len(bits) + 3)

    def rows(k, mask):
        return pl.ds(pl.multiple_of(k * total + flipped(mask) * each, each), each)

    def hop(k, mask, bit):
        src = g.at[rows(k, mask)] if mask else inputs[k]
        return pltpu.make_async_remote_copy(
            src_ref=src, dst_ref=g.at[rows(k, mask)], send_sem=gs.at[k, mask | bit], recv_sem=gr.at[k, mask | bit],
            device_id={"samp": flipped(bit)}, device_id_type=MESH)

    started = []

    def send(k, mask, bit):
        copy = hop(k, mask, bit)
        copy.start()
        started.append(copy)

    def arrive(k, mask):
        pltpu.make_async_remote_copy(
            src_ref=inputs[k], dst_ref=g.at[rows(k, mask)], send_sem=gs.at[k, mask], recv_sem=gr.at[k, mask],
            device_id={"samp": flipped(1)}, device_id_type=MESH).wait_recv()

    for s in range(len(bits)):
        for k in range(2):
            send(k, 0, orders[k][s])
    for k in range(2):
        send(k, 0, 1)
    held = [[0], [0]]
    for s in range(len(bits)):
        for k in range(2):
            new = [m | orders[k][s] for m in held[k]]
            for m in new:
                arrive(k, m)
                for bit in orders[k][s + 1 :]:
                    send(k, m, bit)
                send(k, m, 1)
            held[k] += new
    for k in range(2):
        for m in held[k]:
            arrive(k, m | 1)

    def hop_up(c, d):
        return pltpu.make_async_remote_copy(
            src_ref=sent.at[c, d], dst_ref=below.at[c, d], send_sem=ss.at[c, d], recv_sem=bs.at[c, d],
            device_id={"cpg": lax.min(mz + 1, cpgs - 1)}, device_id_type=MESH)

    def hop_down(c, d):
        return pltpu.make_async_remote_copy(
            src_ref=sent.at[c, d], dst_ref=above.at[c, d], send_sem=ss.at[c, d], recv_sem=us.at[c, d],
            device_id={"cpg": lax.max(mz - 1, 0)}, device_id_type=MESH)

    def own(c, d, k):
        return part[c, pl.ds(pl.multiple_of(k * total + d * block, block), block), :]

    def pass_on(c, d, hop_of, landed, first):
        @pl.when(first)
        def _():
            for k in range(2):
                sent[c, d, pl.ds(k * block, block), :] = own(c, d, k).astype(jnp.bfloat16)

        @pl.when(jnp.logical_not(first))
        def _():
            hop_of(c, d).wait_recv()
            for k in range(2):
                at = pl.ds(k * block, block)
                sent[c, d, at, :] = (own(c, d, k) + landed[c, d, at, :].astype(jnp.float32)).astype(jnp.bfloat16)

        hop_of(c, d).start()

    def turn(t, carry):
        @pl.when(t < chunks)
        def _():
            load(t).wait()
            part[t] = jnp.dot(g[...], v[t], preferred_element_type=jnp.float32)

        cu = t - mz

        @pl.when((cu >= 0) & (cu < chunks))
        def _():
            def body(i, carry):
                pass_on(cu, cpgs - 1 - i, hop_up, below, mz == 0)
                return carry

            lax.fori_loop(0, cpgs - 1 - mz, body, 0)

        cd = t - (cpgs - 1 - mz)

        @pl.when((cd >= 0) & (cd < chunks))
        def _():
            def body(i, carry):
                pass_on(cd, i, hop_down, above, mz == cpgs - 1)
                return carry

            lax.fori_loop(0, mz, body, 0)

        return carry

    lax.fori_loop(0, chunks + cpgs - 1, turn, 0)

    def finish(c, carry):
        cols = pl.ds(pl.multiple_of(c * CHUNK, CHUNK), CHUNK)
        outs = (a_ref, b_ref)
        for k in range(2):
            outs[k][:, cols] = own(c, mz, k)

        @pl.when(mz > 0)
        def _():
            hop_up(c, mz).wait_recv()
            for k in range(2):
                outs[k][:, cols] += below[c, mz, pl.ds(k * block, block), :].astype(jnp.float32)

        @pl.when(mz < cpgs - 1)
        def _():
            hop_down(c, mz).wait_recv()
            for k in range(2):
                outs[k][:, cols] += above[c, mz, pl.ds(k * block, block), :].astype(jnp.float32)

        return carry

    lax.fori_loop(0, chunks, finish, 0)

    def drain(c, carry):
        for d in range(cpgs):
            @pl.when(d != mz)
            def _():
                hop_up(c, d).wait_send()
        return carry

    lax.fori_loop(0, chunks, drain, 0)
    for copy in started:
        copy.wait_send()


def rotate(weighted, design, eigvecs, n, cpgs):
    each, samples = weighted.shape
    comps = eigvecs.shape[1]
    total = each * n
    block = total // cpgs
    chunks = comps // CHUNK
    travel = pltpu.VMEM((chunks, cpgs, 2 * block, CHUNK), jnp.bfloat16)
    piece = pltpu.SemaphoreType.DMA((chunks, cpgs))
    out = jax.ShapeDtypeStruct((block, comps), jnp.float32)
    vmem = pl.BlockSpec(memory_space=pltpu.VMEM)
    return pl.pallas_call(
        functools.partial(rotate_kernel, n, cpgs),
        out_shape=(out, out),
        in_specs=[vmem, vmem, pl.BlockSpec(memory_space=pl.ANY)],
        out_specs=(vmem, vmem),
        scratch_shapes=[
            pltpu.VMEM((2 * total, samples), jnp.bfloat16),
            pltpu.VMEM((chunks, samples, CHUNK), jnp.bfloat16),
            pltpu.VMEM((chunks, 2 * total, CHUNK), jnp.float32),
            travel, travel, travel,
            pltpu.SemaphoreType.DMA((chunks,)),
            pltpu.SemaphoreType.DMA((2, n)),
            pltpu.SemaphoreType.DMA((2, n)),
            piece, piece, piece,
        ],
        compiler_params=pltpu.CompilerParams(collective_id=2, has_side_effects=True, vmem_limit_bytes=60 * 1024 * 1024),
        cost_estimate=pl.CostEstimate(flops=4 * total * samples * comps, bytes_accessed=2 * samples * comps, transcendentals=0),
        name="rotate",
    )(weighted, design, eigvecs)


def band_of(positions, reaches):
    block = reaches.shape[0]
    total = block * lax.axis_size("cpg")
    base = lax.axis_index("cpg") * block
    places = lax.dynamic_slice_in_dim(jnp.pad(positions.astype(jnp.float32), HALO), base, block + 2 * HALO, 0)
    centre = places[HALO : HALO + block]
    index = jnp.arange(2 * HALO + 1, dtype=jnp.int32)[:, None] + jnp.arange(block, dtype=jnp.int32)[None, :]
    near = jnp.stack([places[o : o + block] for o in range(2 * HALO + 1)])
    at = index + base - HALO
    offset = jnp.abs(jnp.arange(2 * HALO + 1, dtype=jnp.int32) - HALO)[:, None]
    keep = (at >= 0) & (at < total) & (offset <= reaches[None, :])
    band = jnp.where(keep, jnp.exp(-jnp.abs(near - centre[None, :]) / band_width), 0.0)
    return jnp.pad(band, ((0, 7), (0, LANES - block)), constant_values=0.0)


def shards(responses, weights, phenotype, eigvecs, eigvals, positions, reaches):
    root_weight = jnp.sqrt(weights.astype(jnp.float32))
    weighted = (root_weight * responses.astype(jnp.float32)).astype(jnp.bfloat16)
    design = (root_weight * phenotype[None, :]).astype(jnp.bfloat16)

    n, cpgs = lax.axis_size("samp"), lax.axis_size("cpg")
    rot_resp, rot_design = rotate(weighted, design, eigvecs, n, cpgs)
    out = fit(rot_resp, rot_design, eigvals[None, :], band_of(positions, reaches), n, cpgs)
    block = reaches.shape[0]
    return (out[0, :block], out[1, :block])


def solution(mesh):
    in_specs = (P("samp", "cpg"), P("samp", "cpg"), P("cpg"), P("cpg", "samp"), P("samp"), P(), P("cpg"))
    out_specs = (P("cpg"), P("cpg"))
    return jax.shard_map(shards, mesh=mesh, in_specs=in_specs, out_specs=out_specs, check_vma=False)
```

```python
import functools

import jax
import jax.numpy as jnp
from jax import lax
from jax.experimental import pallas as pl
from jax.experimental.pallas import tpu as pltpu
from jax.sharding import PartitionSpec as P

ITERS = 4
HALO = 8
EPSILON = 1e-06
band_width = 1000.0
MESH = pl.DeviceIdType.MESH
LANES = 128


def fit_kernel(n, cpgs, a_ref, b_ref, lam_ref, band_ref, out_ref, p_ref, q_ref, r_ref, l_ref, send, recv, edge, zsend, ssem, rsem, esem, fsem):
    me = lax.axis_index("samp")
    mz = lax.axis_index("cpg")
    block = a_ref.shape[0]
    fold = LANES // block
    rows = a_ref.shape[1] // fold
    edge[...] = jnp.zeros_like(edge)

    barrier = pltpu.get_barrier_semaphore()
    for j in range(1, n):
        pl.semaphore_signal(barrier, inc=1, device_id={"samp": lax.rem(me + j, n)}, device_id_type=MESH)

    for other in (lax.rem(mz + 1, cpgs), lax.rem(mz + cpgs - 1, cpgs)):
        pl.semaphore_signal(barrier, inc=1, device_id={"cpg": other}, device_id_type=MESH)

    def folded(ref):
        parts = [ref[:, pl.ds(g * rows, rows)].astype(jnp.float32) for g in range(fold)]
        return jnp.concatenate(parts, axis=0).T

    a = folded(a_ref)
    b = folded(b_ref)
    p_ref[...] = a * b
    q_ref[...] = b * b
    r_ref[...] = a * a
    lam_parts = [jnp.broadcast_to(lam_ref[:, pl.ds(g * rows, rows)], (block, rows)) for g in range(fold)]
    l_ref[...] = jnp.concatenate(lam_parts, axis=0).T

    pl.semaphore_wait(barrier, n + 1)

    step = 64

    def sums(log_scale, full):
        scale = jnp.exp(log_scale)

        def body(i, acc):
            at = pl.ds(pl.multiple_of(i * step, step), step)
            lam = l_ref[at, :]
            inv = 1.0 / (scale * lam + 1.0)
            p = p_ref[at, :]
            q = q_ref[at, :]
            terms = [p * inv, q * inv]
            if full:
                lev = lam * inv
                s = lev * inv
                terms += [lev, lev * lev, s * r_ref[at, :], s * p, s * q]
            terms = [t.reshape(step // 8, 8, LANES).sum(axis=0) for t in terms]
            return tuple(x + y for x, y in zip(acc, terms))

        count = 7 if full else 2
        acc = lax.fori_loop(0, rows // step, body, tuple(jnp.zeros((8, LANES), jnp.float32) for _ in range(count)))
        flat = []
        for x in acc:
            row = jnp.sum(x, axis=0, keepdims=True)
            total = row
            for g in range(1, fold):
                total = total + pltpu.roll(row, g * block, 1)
            flat.append(total)
        flat += [jnp.zeros((1, LANES), jnp.float32)] * (8 - count)
        return jnp.concatenate(flat, axis=0)

    def total(it, value):
        send[it] = value
        copies = []
        for j in range(1, n):
            copies.append(pltpu.make_async_remote_copy(
                src_ref=send.at[it], dst_ref=recv.at[it, j],
                send_sem=ssem.at[it, j], recv_sem=rsem.at[it, j],
                device_id={"samp": lax.rem(me + j, n)}, device_id_type=MESH))
        for c in copies:
            c.start()
        recv[it, 0] = value
        for c in copies:
            c.wait_recv()
        out = jnp.zeros((8, LANES), jnp.float32)
        for d in range(n):
            out = out + recv[it, lax.rem(me - d + n, n)]
        for c in copies:
            c.wait_send()
        return out

    log_scale = jnp.zeros((1, LANES), jnp.float32)
    for it in range(ITERS):
        t = total(it, sums(log_scale, True))
        crossed, energy, traced, fisher = t[0:1], t[1:2] + EPSILON, t[2:3], t[3:4]
        effect = crossed / energy
        spread = t[4:5] - 2.0 * effect * t[5:6] + effect * effect * t[6:7]
        gradient = 0.5 * (spread - traced)
        log_scale = log_scale + jnp.tanh(gradient / (jnp.exp(log_scale) * (0.5 * fisher)))
    t = total(ITERS, sums(log_scale, False))
    z = t[0:1] / jnp.sqrt(t[1:2] + EPSILON)
    z = jnp.broadcast_to(z, (8, LANES))
    zsend[...] = z
    down = pltpu.make_async_remote_copy(
        src_ref=zsend, dst_ref=edge.at[1], send_sem=esem.at[0], recv_sem=fsem.at[1],
        device_id={"cpg": lax.max(mz - 1, 0)}, device_id_type=MESH)
    up = pltpu.make_async_remote_copy(
        src_ref=zsend, dst_ref=edge.at[0], send_sem=esem.at[1], recv_sem=fsem.at[0],
        device_id={"cpg": lax.min(mz + 1, cpgs - 1)}, device_id_type=MESH)

    @pl.when(mz > 0)
    def _():
        down.start()

    @pl.when(mz < cpgs - 1)
    def _():
        up.start()

    @pl.when(mz > 0)
    def _():
        down.wait_send()
        up.wait_recv()

    @pl.when(mz < cpgs - 1)
    def _():
        up.wait_send()
        down.wait_recv()

    lane = lax.broadcasted_iota(jnp.int32, (8, LANES), 1)
    wide = jnp.where(lane < block, z, jnp.where(lane < block + HALO, edge[1], edge[0]))
    acc = jnp.zeros((8, LANES), jnp.float32)
    norm = jnp.zeros((8, LANES), jnp.float32)
    for o in range(2 * HALO + 1):
        shift = (HALO - o) % LANES
        near = pltpu.roll(wide, shift, 1) if shift else wide
        c = band_ref[o : o + 1, :]
        acc = acc + c * near
        norm = norm + c
    row = lax.broadcasted_iota(jnp.int32, (8, LANES), 0)
    out_ref[...] = jnp.where(row == 0, acc / norm, jnp.broadcast_to(log_scale, (8, LANES)))


def fit(a, b, lam, band, n, cpgs):
    block, comps = a.shape
    fold = LANES // block
    rows = comps // fold
    big = pltpu.VMEM((rows, LANES), jnp.float32)
    return pl.pallas_call(
        functools.partial(fit_kernel, n, cpgs),
        out_shape=jax.ShapeDtypeStruct((8, LANES), jnp.float32),
        in_specs=[pl.BlockSpec(memory_space=pltpu.VMEM)] * 4,
        out_specs=pl.BlockSpec(memory_space=pltpu.VMEM),
        scratch_shapes=[
            big, big, big, big,
            pltpu.VMEM((ITERS + 1, 8, LANES), jnp.float32),
            pltpu.VMEM((ITERS + 1, n, 8, LANES), jnp.float32),
            pltpu.VMEM((2, 8, LANES), jnp.float32),
            pltpu.VMEM((8, LANES), jnp.float32),
            pltpu.SemaphoreType.DMA((ITERS + 1, n)),
            pltpu.SemaphoreType.DMA((ITERS + 1, n)),
            pltpu.SemaphoreType.DMA((2,)),
            pltpu.SemaphoreType.DMA((2,)),
        ],
        compiler_params=pltpu.CompilerParams(collective_id=1, has_side_effects=True),
        cost_estimate=pl.CostEstimate(flops=20_000_000, bytes_accessed=2_000_000, transcendentals=0),
        name="fit",
    )(a, b, lam, band)


CHUNK = 256


def rotate_kernel(n, cpgs, w_ref, d_ref, v_hbm, a_ref, b_ref, g, v, part, sent, below, above, vsem, gs, gr, ss, bs, us):
    me = lax.axis_index("samp")
    mz = lax.axis_index("cpg")
    each = w_ref.shape[0]
    total = each * n
    block = total // cpgs
    chunks = v.shape[0]
    units = 2 * chunks
    bits = [1 << i for i in range(1, n.bit_length() - 1)]
    orders = (bits, bits[::-1])
    half = w_ref.shape[1] // 2
    inputs = (w_ref, d_ref)

    def load(c):
        return pltpu.make_async_copy(v_hbm.at[:, pl.ds(pl.multiple_of(c * CHUNK, CHUNK), CHUNK)], v.at[c], vsem.at[c])

    for c in range(chunks):
        load(c).start()

    def flipped(mask):
        out = me
        bit = 1
        while bit <= mask:
            if mask & bit:
                out = out + bit - 2 * bit * lax.rem(lax.div(me, bit), 2)
            bit *= 2
        return out

    barrier = pltpu.get_barrier_semaphore()
    for bit in [1] + bits:
        pl.semaphore_signal(barrier, inc=1, device_id={"samp": flipped(bit)}, device_id_type=MESH)
    for other in (lax.rem(mz + 1, cpgs), lax.rem(mz + cpgs - 1, cpgs)):
        pl.semaphore_signal(barrier, inc=1, device_id={"cpg": other}, device_id_type=MESH)
    for k in range(2):
        g[pl.ds(pl.multiple_of(k * total + me * each, each), each), :] = inputs[k][...]
    pl.semaphore_wait(barrier, len(bits) + 3)

    def rows(k, mask):
        return pl.ds(pl.multiple_of(k * total + flipped(mask) * each, each), each)

    def hop(k, h, mask, bit):
        cols = pl.ds(h * half, half)
        dst = g.at[rows(k, mask), cols]
        return pltpu.make_async_remote_copy(
            src_ref=dst if mask else inputs[k].at[:, cols], dst_ref=dst,
            send_sem=gs.at[k, h, mask | bit], recv_sem=gr.at[k, h, mask | bit],
            device_id={"samp": flipped(bit)}, device_id_type=MESH)

    started = []

    def send(k, h, mask, bit):
        hop(k, h, mask, bit).start()
        started.append((k, h, mask, bit))

    def arrive(k, h, mask):
        cols = pl.ds(h * half, half)
        pltpu.make_async_remote_copy(
            src_ref=inputs[k].at[:, cols], dst_ref=g.at[rows(k, mask), cols],
            send_sem=gs.at[k, h, mask], recv_sem=gr.at[k, h, mask],
            device_id={"samp": flipped(1)}, device_id_type=MESH).wait_recv()

    def begin(k):
        for s in range(len(bits)):
            for h in range(2):
                send(k, h, 0, orders[h][s])
        for h in range(2):
            send(k, h, 0, 1)

    held = [[[0], [0]], [[0], [0]]]

    def relay(k, s):
        for h in range(2):
            new = [m | orders[h][s] for m in held[k][h]]
            for m in new:
                arrive(k, h, m)
                for bit in orders[h][s + 1 :]:
                    send(k, h, m, bit)
                send(k, h, m, 1)
            held[k][h] += new

    def complete(k):
        for h in range(2):
            for m in held[k][h]:
                arrive(k, h, m | 1)

    begin(0)
    for s in range(len(bits) - 1):
        relay(0, s)
    begin(1)
    relay(0, len(bits) - 1)
    complete(0)

    def hop_up(c, d):
        return pltpu.make_async_remote_copy(
            src_ref=sent.at[c, d], dst_ref=below.at[c, d], send_sem=ss.at[c, d], recv_sem=bs.at[c, d],
            device_id={"cpg": lax.min(mz + 1, cpgs - 1)}, device_id_type=MESH)

    def hop_down(c, d):
        return pltpu.make_async_remote_copy(
            src_ref=sent.at[c, d], dst_ref=above.at[c, d], send_sem=ss.at[c, d], recv_sem=us.at[c, d],
            device_id={"cpg": lax.max(mz - 1, 0)}, device_id_type=MESH)

    def own(u, d):
        return part[u, pl.ds(pl.multiple_of(d * block, block), block), :]

    def pass_on(c, d, hop_of, landed, first):
        @pl.when(first)
        def _():
            sent[c, d] = own(c, d).astype(jnp.bfloat16)

        @pl.when(jnp.logical_not(first))
        def _():
            hop_of(c, d).wait_recv()
            sent[c, d] = (own(c, d) + landed[c, d].astype(jnp.float32)).astype(jnp.bfloat16)

        hop_of(c, d).start()

    def turn(t, carry):
        for s in range(len(bits) - 1):
            @pl.when(t == chunks * (s + 1) // len(bits) - 1)
            def _():
                relay(1, s)

        @pl.when(t == chunks)
        def _():
            relay(1, len(bits) - 1)
            complete(1)

        @pl.when(t < chunks)
        def _():
            load(t).wait()

        @pl.when(t < units)
        def _():
            k = lax.div(t, chunks)
            left = g[pl.ds(pl.multiple_of(k * total, total), total), :]
            part[t] = jnp.dot(left, v[t - k * chunks], preferred_element_type=jnp.float32)

        cu = t - mz

        @pl.when((cu >= 0) & (cu < units))
        def _():
            def body(i, carry):
                pass_on(cu, cpgs - 1 - i, hop_up, below, mz == 0)
                return carry

            lax.fori_loop(0, cpgs - 1 - mz, body, 0)

        cd = t - (cpgs - 1 - mz)

        @pl.when((cd >= 0) & (cd < units))
        def _():
            def body(i, carry):
                pass_on(cd, i, hop_down, above, mz == cpgs - 1)
                return carry

            lax.fori_loop(0, mz, body, 0)

        return carry

    lax.fori_loop(0, units + cpgs - 1, turn, 0)

    def finish(c, carry):
        cols = pl.ds(pl.multiple_of(c * CHUNK, CHUNK), CHUNK)
        for k, out in enumerate((a_ref, b_ref)):
            u = k * chunks + c
            out[:, cols] = own(u, mz)

            @pl.when(mz > 0)
            def _():
                hop_up(u, mz).wait_recv()
                out[:, cols] += below[u, mz].astype(jnp.float32)

            @pl.when(mz < cpgs - 1)
            def _():
                hop_down(u, mz).wait_recv()
                out[:, cols] += above[u, mz].astype(jnp.float32)

        return carry

    lax.fori_loop(0, chunks, finish, 0)

    def drain(c, carry):
        for d in range(cpgs):
            @pl.when(d != mz)
            def _():
                hop_up(c, d).wait_send()
        return carry

    lax.fori_loop(0, units, drain, 0)
    for item in started:
        hop(*item).wait_send()


def rotate(weighted, design, eigvecs, n, cpgs):
    each, samples = weighted.shape
    comps = eigvecs.shape[1]
    total = each * n
    block = total // cpgs
    chunks = comps // CHUNK
    travel = pltpu.VMEM((2 * chunks, cpgs, block, CHUNK), jnp.bfloat16)
    piece = pltpu.SemaphoreType.DMA((2 * chunks, cpgs))
    out = jax.ShapeDtypeStruct((block, comps), jnp.float32)
    vmem = pl.BlockSpec(memory_space=pltpu.VMEM)
    return pl.pallas_call(
        functools.partial(rotate_kernel, n, cpgs),
        out_shape=(out, out),
        in_specs=[vmem, vmem, pl.BlockSpec(memory_space=pl.ANY)],
        out_specs=(vmem, vmem),
        scratch_shapes=[
            pltpu.VMEM((2 * total, samples), jnp.bfloat16),
            pltpu.VMEM((chunks, samples, CHUNK), jnp.bfloat16),
            pltpu.VMEM((2 * chunks, total, CHUNK), jnp.float32),
            travel, travel, travel,
            pltpu.SemaphoreType.DMA((chunks,)),
            pltpu.SemaphoreType.DMA((2, 2, n)),
            pltpu.SemaphoreType.DMA((2, 2, n)),
            piece, piece, piece,
        ],
        compiler_params=pltpu.CompilerParams(collective_id=2, has_side_effects=True, vmem_limit_bytes=60 * 1024 * 1024),
        cost_estimate=pl.CostEstimate(flops=4 * total * samples * comps, bytes_accessed=2 * samples * comps, transcendentals=0),
        name="rotate",
    )(weighted, design, eigvecs)


def band_of(positions, reaches):
    block = reaches.shape[0]
    total = block * lax.axis_size("cpg")
    base = lax.axis_index("cpg") * block
    places = lax.dynamic_slice_in_dim(jnp.pad(positions.astype(jnp.float32), HALO), base, block + 2 * HALO, 0)
    centre = places[HALO : HALO + block]
    index = jnp.arange(2 * HALO + 1, dtype=jnp.int32)[:, None] + jnp.arange(block, dtype=jnp.int32)[None, :]
    near = jnp.stack([places[o : o + block] for o in range(2 * HALO + 1)])
    at = index + base - HALO
    offset = jnp.abs(jnp.arange(2 * HALO + 1, dtype=jnp.int32) - HALO)[:, None]
    keep = (at >= 0) & (at < total) & (offset <= reaches[None, :])
    band = jnp.where(keep, jnp.exp(-jnp.abs(near - centre[None, :]) / band_width), 0.0)
    return jnp.pad(band, ((0, 7), (0, LANES - block)), constant_values=0.0)


def shards(responses, weights, phenotype, eigvecs, eigvals, positions, reaches):
    root_weight = jnp.sqrt(weights.astype(jnp.float32))
    weighted = (root_weight * responses.astype(jnp.float32)).astype(jnp.bfloat16)
    design = (root_weight * phenotype[None, :]).astype(jnp.bfloat16)

    n, cpgs = lax.axis_size("samp"), lax.axis_size("cpg")
    rot_resp, rot_design = rotate(weighted, design, eigvecs, n, cpgs)
    out = fit(rot_resp, rot_design, eigvals[None, :], band_of(positions, reaches), n, cpgs)
    block = reaches.shape[0]
    return (out[0, :block], out[1, :block])


def solution(mesh):
    in_specs = (P("samp", "cpg"), P("samp", "cpg"), P("cpg"), P("cpg", "samp"), P("samp"), P(), P("cpg"))
    out_specs = (P("cpg"), P("cpg"))
    return jax.shard_map(shards, mesh=mesh, in_specs=in_specs, out_specs=out_specs, check_vma=False)
```
